32 devices in a mesh: seq: 8 (over z, x), head: 4 (over y, core).
Axes of the slice: x: 2, y: 2, z: 4, core: 2. Of those that a mesh axis runs over, the one named last changes fastest.
Arguments:
- queries: bfloat16 [2048, 2048], P('seq', 'head'), may hold values from -8 to 8
- keys: bfloat16 [2048, 512], P('seq', 'head'), may hold values from -4 to 4
- values: bfloat16 [2048, 512], P('seq', 'head'), may hold values from -6 to 6
- doc_ids: int32 [2048], replicated, may hold values from 0 to 15, never falling along the last dimension, each value on 1 to 1024 neighbouring positions
- span_order: int32 [16], replicated, may hold values from 0 to 15, each once
- out_weight: bfloat16 [2048, 4096], P('head', 'seq'), may hold values from -0.1875 to 0.1875
Outputs:
- layer_out: bfloat16 [2048, 4096], P('seq', 'head')
The draws below stay inside these ranges and needn't reach their ends.
All inputs are finite; a program needn't handle non-finite values.
Results may differ from the reference program's by a relative error of at most 0.012.
Values may be sent and summed in bfloat16 or wider, within the bound.
A program may use at most 64 MiB of HBM per device.

```python
import math
import jax
import jax.numpy as jnp
import numpy as np
from jax import lax

D = 4096
HEADS = 16
KV_HEADS = 4
DH = 128
GROUP = 4
TOK_DEV = 256
SEQ = 2048
DOCS = 16
MAX_DOC = 1024
N_SEQ = 8


def draw_queries(key, part):
    base = jnp.clip(jax.random.normal(jax.random.fold_in(key, 11), (SEQ, HEADS * DH), jnp.float32), -4.0, 4.0)
    return base.astype(jnp.bfloat16)


def draw_keys(key, part):
    base = jnp.clip(jax.random.normal(jax.random.fold_in(key, 21), (SEQ, KV_HEADS * DH), jnp.float32), -4.0, 4.0)
    return base.astype(jnp.bfloat16)


def spiked(result, key, source, target, parts, factor):
    owner, partner = [(jnp.arange(result.shape[dim]) // (result.shape[dim] // parts)).reshape([-1 if axis == dim else 1 for axis in range(result.ndim)]) for dim in (source, target)]
    chosen = jax.random.permutation(key, parts)[partner]
    strong = (owner == chosen) | (owner == (partner + parts // 2) % parts)
    return jnp.where(strong, factor * result, result)


def block_scale(own_key, shape, pieces, least, high):
    def one(axis_at, shards_of):
        steps = jax.random.uniform(jax.random.fold_in(jax.random.fold_in(own_key, 6), axis_at), (shards_of,), jnp.float32, least / len(pieces), high / len(pieces))
        return jnp.repeat(jnp.exp(steps), shape[axis_at] // shards_of).reshape((-1,) + (1,) * (len(shape) - axis_at - 1))

    level = one(*pieces[0])
    for cut in pieces[1:]:
        level = level * one(*cut)
    return level


def length_profile(amount, total, limit, lean):
    loads = [(1 << 20) // math.isqrt(grade ** lean) + 1 for grade in range(2, amount + 1)]
    surplus, given = total - limit - (amount - 1), [1] * (amount - 1)
    while surplus > 0:
        candidates = [i for i in range(amount - 1) if given[i] < limit]
        whole, remaining = sum([loads[i] for i in candidates]), surplus
        for i in candidates:
            more = min(limit - given[i], max(1, remaining * loads[i] // whole), surplus)
            given[i] = given[i] + more
            surplus = surplus - more
    return np.array([limit] + given)


def ragged_sizes(stream_key, amount, total, most, lean):
    if amount == 2:
        one = jax.random.randint(stream_key, (), max(1, total - most), min(most, total - 1) + 1)
        return jnp.stack([one, total - one])
    tallies = jnp.asarray(length_profile(amount, total, most, lean), jnp.int32)
    pairs = (amount - 1) // 2
    donor, taker = tallies[1:1 + 2 * pairs:2], tallies[2:2 + 2 * pairs:2]
    slack = jnp.minimum(donor - 1, most - taker)
    shifted = jax.random.randint(jax.random.fold_in(stream_key, 1), (pairs,), 0, 1 << 20) % (slack + 1)
    tallies = tallies.at[1:1 + 2 * pairs:2].set(donor - shifted).at[2:2 + 2 * pairs:2].set(taker + shifted)
    return tallies[jax.random.permutation(jax.random.fold_in(stream_key, 2), amount)]


def centred(rng, dims, width, bound, cuts=(), kind=jnp.bfloat16):
    entries = jax.random.normal(rng, dims, jnp.float32) * width
    if len(cuts) > 0:
        entries = block_scale(rng, dims, cuts, -0.22, 0.18) * entries
    return jnp.clip(entries, min=-bound, max=bound).astype(kind)


def noise_with(own_key, shape, spread, reach, split, heavy, kind=jnp.bfloat16):
    values = spread * jax.random.normal(own_key, shape, jnp.float32)
    if split:
        values = values * block_scale(own_key, shape, split, -0.22, 0.18)
    return jnp.clip(spiked(values, jax.random.fold_in(own_key, 3), *heavy), -reach, reach).astype(kind)


def setup_inputs(seed: int = 0) -> dict:
    arg_keys = jax.random.split(jax.random.key(seed), 7)
    return {
        "queries": draw_queries(jax.random.fold_in(arg_keys[6], 71), 0),
        "keys": draw_keys(jax.random.fold_in(arg_keys[6], 71), 0),
        "values": centred(arg_keys[2], (SEQ, KV_HEADS * DH), 1.0, 6.0, ((0, 8), (1, 4))),
        "doc_ids": jnp.searchsorted(jnp.cumsum(ragged_sizes(arg_keys[3], DOCS, SEQ, MAX_DOC, 2)), jnp.arange(SEQ), side="right").astype(jnp.int32),
        "span_order": jax.random.permutation(arg_keys[4], 2 * N_SEQ).astype(jnp.int32),
        "out_weight": noise_with(arg_keys[5], (HEADS * DH, D), (HEADS * DH) ** -0.5, 0.1875, ((0, 4), (1, 8)), (0, 1, 8, 2.0)),
    }


def reference(queries, keys, values, doc_ids, span_order, out_weight):
    span = TOK_DEV // 2
    rows = jnp.arange(SEQ, dtype=jnp.int32)
    pos = (span_order[rows // span] * span + rows % span).astype(jnp.int32)
    doc = doc_ids[pos]
    scale = 1.0 / math.sqrt(DH)
    key_all = keys.reshape(SEQ, KV_HEADS, DH).astype(jnp.float32)
    val_all = values.reshape(SEQ, KV_HEADS, DH).astype(jnp.float32)
    block = math.gcd(SEQ, 128)

    def one_block(index):
        start = (index * block).astype(jnp.int32)
        qblk = lax.dynamic_slice_in_dim(queries, start, block, 0)
        qblk = qblk.reshape(block, KV_HEADS, GROUP, DH).astype(jnp.float32)
        qpos = lax.dynamic_slice_in_dim(pos, start, block, 0)
        qdoc = lax.dynamic_slice_in_dim(doc, start, block, 0)
        scores = jnp.einsum('qhgd,khd->hgqk', qblk, key_all) * scale
        visible = (qdoc[:, None] == doc[None, :]) & (pos[None, :] <= qpos[:, None])
        masked = jnp.where(visible, scores, jnp.float32(-1e+30))
        largest = lax.optimization_barrier(jnp.max(masked, axis=-1, keepdims=True))
        weights = jnp.where(visible, jnp.exp(masked - largest), jnp.float32(0.0))
        total = lax.optimization_barrier(jnp.sum(weights, axis=-1))
        weights_b = weights.astype(jnp.bfloat16).astype(jnp.float32)
        summed = jnp.einsum('hgqk,khd->qhgd', weights_b, val_all)
        attended = summed / jnp.transpose(total, (2, 0, 1))[..., None]
        return attended.astype(jnp.bfloat16).reshape(block, HEADS * DH)
    attended = lax.map(one_block, jnp.arange(SEQ // block, dtype=jnp.int32))
    attended = attended.reshape(SEQ, HEADS * DH)
    return jnp.dot(attended, out_weight, preferred_element_type=jnp.float32).astype(jnp.bfloat16)
```

```python
import functools
import math

import jax
import jax.numpy as jnp
from jax import lax
from jax.experimental import pallas as pl
from jax.experimental.pallas import tpu as pltpu
from jax.sharding import PartitionSpec as P

MESH = pl.DeviceIdType.MESH

DH = 128


def gathered_form(queries, keys, values, doc_ids, span_order, out_weight):
    tok_rows = queries.shape[0]
    span = tok_rows // 2
    local_heads = queries.shape[1] // DH
    local_kv = keys.shape[1] // DH
    group_size = local_heads // local_kv
    n_blocks = span_order.shape[0]
    scale = 1.0 / math.sqrt(DH)
    mine = lax.axis_index("seq")
    own_blocks = lax.dynamic_slice_in_dim(span_order, 2 * mine, 2, 0)
    local_rows = jnp.arange(tok_rows, dtype=jnp.int32)
    qpos = jnp.where(local_rows < span, own_blocks[0], own_blocks[1]) * span + local_rows % span
    qdoc = jnp.take(doc_ids, qpos)
    q_heads = queries.reshape(tok_rows, local_kv, group_size, DH)

    def update(state, kblk, vblk, kpos, kdoc):
        largest, total, summed = state
        count = kblk.shape[0]
        k_heads = kblk.reshape(count, local_kv, DH)
        v_heads = vblk.reshape(count, local_kv, DH)
        scores = (
            jnp.einsum("qhgd,khd->hgqk", q_heads, k_heads, preferred_element_type=jnp.float32)
            * scale
        )
        visible = (qdoc[:, None] == kdoc[None, :]) & (kpos[None, :] <= qpos[:, None])
        masked = jnp.where(visible, scores, jnp.float32(-1e30))
        new_largest = jnp.maximum(largest, jnp.max(masked, axis=-1))
        factor = jnp.exp(largest - new_largest)
        weights = jnp.where(visible, jnp.exp(masked - new_largest[..., None]), jnp.float32(0.0))
        total = total * factor + jnp.sum(weights, axis=-1)
        weights_b = weights.astype(jnp.bfloat16)
        added = jnp.einsum("hgqk,khd->qhgd", weights_b, v_heads, preferred_element_type=jnp.float32)
        summed = summed * jnp.transpose(factor, (2, 0, 1))[..., None] + added
        return (new_largest, total, summed)

    initial = (
        jnp.full((local_kv, group_size, tok_rows), -1e30, jnp.float32),
        jnp.zeros((local_kv, group_size, tok_rows), jnp.float32),
        jnp.zeros((tok_rows, local_kv, group_size, DH), jnp.float32),
    )
    state = initial
    kpiece = lax.all_gather(keys, "seq", axis=0, tiled=True)
    vpiece = lax.all_gather(values, "seq", axis=0, tiled=True)
    count = kpiece.shape[0]
    width = math.gcd(count, 1024)
    steps = count // width
    rows = jnp.arange(count, dtype=jnp.int32)
    match = (rows // span)[:, None] == jnp.arange(n_blocks, dtype=jnp.int32)[None, :]
    owner = jnp.sum(jnp.where(match, span_order[None, :], 0), axis=1)
    kpos = owner * span + rows % span
    kdoc = jnp.take(doc_ids, kpos)
    kparts = kpiece.reshape(steps, width, kpiece.shape[1])
    vparts = vpiece.reshape(steps, width, vpiece.shape[1])

    def one_step(carry, items):
        kblk, vblk, pblk, dblk = items
        carry = update(carry, kblk, vblk, pblk, dblk)
        return (carry, None)

    state, unused = lax.scan(
        one_step, state, (kparts, vparts, kpos.reshape(steps, width), kdoc.reshape(steps, width))
    )
    largest, total, summed = state
    attended = (summed / jnp.transpose(total, (2, 0, 1))[..., None]).astype(jnp.bfloat16)
    attended = attended.reshape(tok_rows, local_heads * DH)
    partial_out = jnp.dot(
        attended,
        lax.all_gather(out_weight, "seq", axis=1, tiled=True),
        preferred_element_type=jnp.float32,
    )
    return lax.psum_scatter(
        partial_out.astype(jnp.bfloat16), "head", scatter_dimension=1, tiled=True
    )


def ring_kernel(
    n, q_ref, k_ref, v_ref, doc_ref, order_ref, w_ref, out_ref,
    kbuf, vbuf, wbuf, bias, att, stage, kept, sums,
    k_send, k_recv, v_send, v_recv, w_send, w_recv, half_send, half_recv,
    att_send, att_recv, sum_send, sum_recv,
):
    seq = lax.axis_index("seq")
    head = lax.axis_index("head")
    pair, core = head // 2, head % 2
    partner = 2 * pair + 1 - core
    last = n // 2
    rows = q_ref.shape[0]
    span = rows // 2
    heads = q_ref.shape[1] // DH
    depth, width = w_ref.shape
    half = width // 2
    piece = depth // 2
    pieces = 4
    scale = 1.0 / math.sqrt(DH)

    def seq_at(place):
        low = place // last
        return (1 - low) * 2 * place + low * (2 * (n - 1 - place) + 1)

    odd = seq % 2
    place = (1 - odd) * (seq // 2) + odd * (n - 1 - seq // 2)
    right, left = seq_at((place + 1) % n), seq_at((place + n - 1) % n)
    ring = ({"seq": right}, {"seq": left})

    def slot(way, dist):
        if dist == 0:
            return 0
        if dist == last:
            return n - 1
        return dist if way == 0 else last - 1 + dist

    def origin(number):
        if number < last:
            return seq_at((place + n - number) % n)
        if number == n - 1:
            return seq_at((place + last) % n)
        return seq_at((place + number - last + 1) % n)

    barrier = pltpu.get_barrier_semaphore()
    other = (pair + 1) % 2
    greet = ring + ({"head": partner}, {"head": 2 * other}, {"head": 2 * other + 1})
    for device in greet:
        pl.semaphore_signal(barrier, inc=1, device_id=device, device_id_type=MESH)
    pl.semaphore_wait(barrier, len(greet))

    sent = []

    def start(copy):
        copy.start()
        sent.append(copy)

    def remote(src, dst, send, recv, device):
        return pltpu.make_async_remote_copy(
            src_ref=src, dst_ref=dst, send_sem=send, recv_sem=recv, device_id=device, device_id_type=MESH
        )

    def kv_copy(which, way, dist):
        own, buf, ss, rs = ((k_ref, kbuf, k_send, k_recv), (v_ref, vbuf, v_send, v_recv))[which]
        src = own if dist == 1 else buf.at[slot(way, dist - 1)]
        to = slot(way, dist)
        return remote(src, buf.at[to], ss.at[way, dist], rs.at[to], ring[way])

    def kv_goes(which, way, dist):
        return dist < last or (dist == last and which == way)

    mine = pl.ds(pl.multiple_of(core * half, half), half)
    theirs = pl.ds(pl.multiple_of((1 - core) * half, half), half)

    def w_copy(way, dist, number):
        part, cut = number // 2, number % 2
        cut_rows = pl.ds(cut * piece, piece)
        if dist == 1 and part == 0:
            src = w_ref.at[cut_rows, mine]
        else:
            src = wbuf.at[slot(way, dist - 1), part, cut_rows]
        to = slot(way, dist)
        return remote(
            src, wbuf.at[to, part, cut_rows], w_send.at[way, dist, number], w_recv.at[to, number], ring[way]
        )

    def w_goes(way, dist, number):
        return dist < last or (dist == last and number // 2 == way)

    def half_copy(cut):
        cut_rows = pl.ds(cut * piece, piece)
        return remote(
            w_ref.at[cut_rows, theirs], wbuf.at[0, 1, cut_rows], half_send.at[cut], half_recv.at[cut], {"head": partner}
        )

    def send_kv(dist):
        for way in range(2):
            for which in range(2):
                if kv_goes(which, way, dist):
                    start(kv_copy(which, way, dist))

    def wait_kv(dist):
        for way in range(2):
            for which in range(2):
                if kv_goes(which, way, dist):
                    kv_copy(which, way, dist).wait_recv()

    def send_w(dist, number):
        for way in range(2):
            if w_goes(way, dist, number):
                start(w_copy(way, dist, number))

    def pass_w(dist, number):
        for way in range(2):
            if w_goes(way, dist, number):
                w_copy(way, dist, number).wait_recv()
                if w_goes(way, dist + 1, number):
                    start(w_copy(way, dist + 1, number))

    send_kv(1)
    send_w(1, 0)
    for cut in range(2):
        start(half_copy(cut))
    send_w(1, 1)
    kbuf[0] = k_ref[...]
    vbuf[0] = v_ref[...]
    wbuf[0, 0] = w_ref[:, mine]
    for cut in range(2):
        half_copy(cut).wait_recv()

    down = lax.broadcasted_iota(jnp.int32, (span, span), 0)
    along = lax.broadcasted_iota(jnp.int32, (span, span), 1)
    query_at, query_doc = [], []
    for part in range(2):
        block = order_ref[2 * seq + part]
        query_at.append(down + block * span)
        docs = doc_ref[pl.ds(block, 1), :].astype(jnp.float32)
        query_doc.append(jnp.transpose(jnp.broadcast_to(docs, (span, span))))

    def mask(number):
        for j in range(2):
            block = order_ref[2 * origin(number) + j]
            docs = doc_ref[pl.ds(block, 1), :].astype(jnp.float32)
            key_at = along + block * span
            first = (2 * number + j) * span
            for part in range(2):
                seen = (query_doc[part] == docs) & (key_at <= query_at[part])
                bias[part, :, first : first + span] = jnp.where(seen, jnp.float32(0.0), jnp.float32(-1e30))

    mask(0)
    for dist in range(1, last + 1):
        wait_kv(dist)
        if dist < last:
            send_kv(dist + 1)
        if dist + 1 < pieces:
            send_w(1, dist + 1)
        mask(slot(0, dist))
        if dist < last:
            mask(slot(1, dist))
    for number in range(dist + 1, pieces):
        send_w(1, number)

    def attend(part, h):
        q = q_ref[part * span : (part + 1) * span, h * DH : (h + 1) * DH]
        keys = kbuf[...].reshape(n * rows, DH)
        scores = lax.dot_general(q, keys, (((1,), (1,)), ((), ())), preferred_element_type=jnp.float32)
        masked = scores * scale + bias[part]
        weights = jnp.exp(masked - jnp.max(masked, axis=-1, keepdims=True))
        total = jnp.sum(weights, axis=-1, keepdims=True)
        summed = jnp.dot(
            weights.astype(jnp.bfloat16), vbuf[...].reshape(n * rows, DH), preferred_element_type=jnp.float32
        )
        att[0, part * span : (part + 1) * span, h * DH : (h + 1) * DH] = (summed / total).astype(jnp.bfloat16)

    units = [(part, h) for part in range(2) for h in range(heads)]
    events = [(dist, number) for dist in range(1, last + 1) for number in range(pieces)]
    cols_of = out_ref.shape[1] // width

    def target(number):
        block = origin(number)
        to = block // cols_of
        return block, to, 2 * ((pair + to // 2) % 2) + (core + to) % 2

    def sum_copy(number):
        block, to, code = target(number)
        return remote(
            stage.at[number],
            sums.at[code, block % cols_of],
            sum_send.at[number],
            sum_recv.at[code, block % cols_of],
            {"head": to},
        )

    def project(number):
        block, to, code = target(number)
        added = jnp.dot(att[0], wbuf[number, 0], preferred_element_type=jnp.float32)
        added = added + jnp.dot(att[1], wbuf[number, 1], preferred_element_type=jnp.float32)

        @pl.when(code == 0)
        def _():
            kept[block % cols_of] = added

        @pl.when(code != 0)
        def _():
            stage[number] = added.astype(jnp.bfloat16)
            sum_copy(number).start()

    def att_copy():
        return remote(att.at[0], att.at[1], att_send, att_recv, {"head": partner})

    ready = [0]
    done_att = False
    for at, (dist, number) in enumerate(events):
        pass_w(dist, number)
        if number == pieces - 1:
            ready += [slot(0, dist)] + ([slot(1, dist)] if dist < last else [])
        if at >= pieces - 1:
            for part, h in units[:2]:
                attend(part, h)
            units = units[2:]
        if not units and not done_att:
            start(att_copy())
            att_copy().wait_recv()
            done_att = True
        elif done_att and at < len(events) - 1:
            for _ in range(2):
                if ready:
                    project(ready.pop(0))
    for number in ready:
        project(number)

    own = pl.multiple_of(core * half, half)
    far = pl.multiple_of((1 - core) * half, half)
    for j in range(cols_of):
        for code in range(1, 4):
            remote(stage.at[0], sums.at[code, j], sum_send.at[0], sum_recv.at[code, j], {"head": partner}).wait_recv()
        out_ref[:, pl.ds(j * width + own, half)] = (kept[j] + sums[2, j].astype(jnp.float32)).astype(jnp.bfloat16)
        out_ref[:, pl.ds(j * width + far, half)] = (
            sums[1, j].astype(jnp.float32) + sums[3, j].astype(jnp.float32)
        ).astype(jnp.bfloat16)
    for copy in sent:
        copy.wait_send()
    for number in range(n):

        @pl.when(target(number)[2] != 0)
        def _(number=number):
            sum_copy(number).wait_send()


def ring_form(n, queries, keys, values, doc_ids, span_order, out_weight):
    rows = queries.shape[0]
    depth, width = out_weight.shape
    half = width // 2
    per_head = n // 4
    bf16 = jnp.bfloat16
    vmem = pl.BlockSpec(memory_space=pltpu.VMEM)
    dma = pltpu.SemaphoreType.DMA
    return pl.pallas_call(
        functools.partial(ring_kernel, n),
        out_shape=jax.ShapeDtypeStruct((rows, width * per_head), bf16),
        in_specs=[vmem, vmem, vmem, vmem, pl.BlockSpec(memory_space=pltpu.SMEM), vmem],
        out_specs=vmem,
        scratch_shapes=[
            pltpu.VMEM((n, rows, DH), bf16),
            pltpu.VMEM((n, rows, DH), bf16),
            pltpu.VMEM((n, 2, depth, half), bf16),
            pltpu.VMEM((2, rows // 2, n * rows), jnp.float32),
            pltpu.VMEM((2,) + queries.shape, bf16),
            pltpu.VMEM((n, rows, half), bf16),
            pltpu.VMEM((per_head, rows, half), jnp.float32),
            pltpu.VMEM((4, per_head, rows, half), bf16),
            dma((2, n // 2 + 1)),
            dma((n,)),
            dma((2, n // 2 + 1)),
            dma((n,)),
            dma((2, n // 2 + 1, 4)),
            dma((n, 4)),
            dma((2,)),
            dma((2,)),
            dma,
            dma,
            dma((n,)),
            dma((4, per_head)),
        ],
        compiler_params=pltpu.CompilerParams(
            collective_id=0, has_side_effects=True, vmem_limit_bytes=48 * 1024 * 1024
        ),
    )(queries, keys, values, doc_ids.reshape(-1, rows // 2), span_order, out_weight)


def on_device(mesh_shape, queries, keys, values, doc_ids, span_order, out_weight):
    n, groups = mesh_shape["seq"], mesh_shape["head"]
    rows = queries.shape[0]
    depth, width = out_weight.shape
    held = n * (depth * width + 2 * rows * DH) * 2
    fits = (
        groups == 4
        and n % 4 == 0
        and rows == 2 * DH
        and keys.shape[1] == DH
        and width % (2 * DH) == 0
        and held <= 16 * 1024 * 1024
    )
    if fits:
        return ring_form(n, queries, keys, values, doc_ids, span_order, out_weight)
    return gathered_form(queries, keys, values, doc_ids, span_order, out_weight)


def solution(mesh):
    return jax.shard_map(
        functools.partial(on_device, dict(mesh.shape)),
        mesh=mesh,
        in_specs=(P("seq", "head"), P("seq", "head"), P("seq", "head"), P(), P(), P("head", "seq")),
        out_specs=P("seq", "head"),
        check_vma=False,
    )
```

```python
import functools
import math

import jax
import jax.numpy as jnp
from jax import lax
from jax.experimental import pallas as pl
from jax.experimental.pallas import tpu as pltpu
from jax.sharding import PartitionSpec as P

MESH = pl.DeviceIdType.MESH

DH = 128


def gathered_form(queries, keys, values, doc_ids, span_order, out_weight):
    tok_rows = queries.shape[0]
    span = tok_rows // 2
    local_heads = queries.shape[1] // DH
    local_kv = keys.shape[1] // DH
    group_size = local_heads // local_kv
    n_blocks = span_order.shape[0]
    scale = 1.0 / math.sqrt(DH)
    mine = lax.axis_index("seq")
    own_blocks = lax.dynamic_slice_in_dim(span_order, 2 * mine, 2, 0)
    local_rows = jnp.arange(tok_rows, dtype=jnp.int32)
    qpos = jnp.where(local_rows < span, own_blocks[0], own_blocks[1]) * span + local_rows % span
    qdoc = jnp.take(doc_ids, qpos)
    q_heads = queries.reshape(tok_rows, local_kv, group_size, DH)

    def update(state, kblk, vblk, kpos, kdoc):
        largest, total, summed = state
        count = kblk.shape[0]
        k_heads = kblk.reshape(count, local_kv, DH)
        v_heads = vblk.reshape(count, local_kv, DH)
        scores = (
            jnp.einsum("qhgd,khd->hgqk", q_heads, k_heads, preferred_element_type=jnp.float32)
            * scale
        )
        visible = (qdoc[:, None] == kdoc[None, :]) & (kpos[None, :] <= qpos[:, None])
        masked = jnp.where(visible, scores, jnp.float32(-1e30))
        new_largest = jnp.maximum(largest, jnp.max(masked, axis=-1))
        factor = jnp.exp(largest - new_largest)
        weights = jnp.where(visible, jnp.exp(masked - new_largest[..., None]), jnp.float32(0.0))
        total = total * factor + jnp.sum(weights, axis=-1)
        weights_b = weights.astype(jnp.bfloat16)
        added = jnp.einsum("hgqk,khd->qhgd", weights_b, v_heads, preferred_element_type=jnp.float32)
        summed = summed * jnp.transpose(factor, (2, 0, 1))[..., None] + added
        return (new_largest, total, summed)

    initial = (
        jnp.full((local_kv, group_size, tok_rows), -1e30, jnp.float32),
        jnp.zeros((local_kv, group_size, tok_rows), jnp.float32),
        jnp.zeros((tok_rows, local_kv, group_size, DH), jnp.float32),
    )
    state = initial
    kpiece = lax.all_gather(keys, "seq", axis=0, tiled=True)
    vpiece = lax.all_gather(values, "seq", axis=0, tiled=True)
    count = kpiece.shape[0]
    width = math.gcd(count, 1024)
    steps = count // width
    rows = jnp.arange(count, dtype=jnp.int32)
    match = (rows // span)[:, None] == jnp.arange(n_blocks, dtype=jnp.int32)[None, :]
    owner = jnp.sum(jnp.where(match, span_order[None, :], 0), axis=1)
    kpos = owner * span + rows % span
    kdoc = jnp.take(doc_ids, kpos)
    kparts = kpiece.reshape(steps, width, kpiece.shape[1])
    vparts = vpiece.reshape(steps, width, vpiece.shape[1])

    def one_step(carry, items):
        kblk, vblk, pblk, dblk = items
        carry = update(carry, kblk, vblk, pblk, dblk)
        return (carry, None)

    state, unused = lax.scan(
        one_step, state, (kparts, vparts, kpos.reshape(steps, width), kdoc.reshape(steps, width))
    )
    largest, total, summed = state
    attended = (summed / jnp.transpose(total, (2, 0, 1))[..., None]).astype(jnp.bfloat16)
    attended = attended.reshape(tok_rows, local_heads * DH)
    partial_out = jnp.dot(
        attended,
        lax.all_gather(out_weight, "seq", axis=1, tiled=True),
        preferred_element_type=jnp.float32,
    )
    return lax.psum_scatter(
        partial_out.astype(jnp.bfloat16), "head", scatter_dimension=1, tiled=True
    )


def ring_kernel(
    n, q_in, k_in, v_in, doc_in, order_in, w_in, out_ref,
    q_ref, doc_ref, order_ref, w_out, fetched, kbuf, vbuf, wbuf, bias, att, stage, kept, sums,
    k_send, k_recv, v_send, v_recv, w_send, w_recv, half_send, half_recv,
    att_send, att_recv, sum_send, sum_recv,
):
    seq = lax.axis_index("seq")
    head = lax.axis_index("head")
    pair, core = head // 2, head % 2
    partner = 2 * pair + 1 - core
    last = n // 2
    rows = q_ref.shape[0]
    span = rows // 2
    heads = q_ref.shape[1] // DH
    width = w_in.shape[1]
    half = width // 2
    quarter = half // 2
    pieces = (0, 2, 1, 3)
    scale = 1.0 / math.sqrt(DH)

    def seq_at(place):
        low = place // last
        return (1 - low) * 2 * place + low * (2 * (n - 1 - place) + 1)

    odd = seq % 2
    place = (1 - odd) * (seq // 2) + odd * (n - 1 - seq // 2)
    right, left = seq_at((place + 1) % n), seq_at((place + n - 1) % n)
    ring = ({"seq": right}, {"seq": left})

    def slot(way, dist):
        if dist == 0:
            return 0
        if dist == last:
            return n - 1
        return dist if way == 0 else last - 1 + dist

    def origin(number):
        if number < last:
            return seq_at((place + n - number) % n)
        if number == n - 1:
            return seq_at((place + last) % n)
        return seq_at((place + number - last + 1) % n)

    mine = pl.ds(pl.multiple_of(core * half, half), half)
    theirs = pl.ds(pl.multiple_of((1 - core) * half, half), half)
    fetches = [
        pltpu.make_async_copy(src, dst, fetched.at[at])
        for at, (src, dst) in enumerate(
            (
                (k_in, kbuf.at[0]),
                (v_in, vbuf.at[0]),
                (w_in.at[:, theirs], w_out),
                (w_in.at[:, mine], wbuf.at[0, 0]),
                (doc_in, doc_ref),
                (order_in, order_ref),
                (q_in, q_ref),
            )
        )
    ]
    for fetch in fetches:
        fetch.start()

    barrier = pltpu.get_barrier_semaphore()
    other = (pair + 1) % 2
    greet = ring + ({"head": partner}, {"head": 2 * other}, {"head": 2 * other + 1})
    for device in greet:
        pl.semaphore_signal(barrier, inc=1, device_id=device, device_id_type=MESH)
    pl.semaphore_wait(barrier, len(greet))

    sent = []

    def start(copy):
        copy.start()
        sent.append(copy)

    def remote(src, dst, send, recv, device):
        return pltpu.make_async_remote_copy(
            src_ref=src, dst_ref=dst, send_sem=send, recv_sem=recv, device_id=device, device_id_type=MESH
        )

    def kv_copy(which, way, dist):
        buf, ss, rs = ((kbuf, k_send, k_recv), (vbuf, v_send, v_recv))[which]
        to = slot(way, dist)
        return remote(buf.at[slot(way, dist - 1)], buf.at[to], ss.at[way, dist], rs.at[to], ring[way])

    def kv_goes(which, way, dist):
        return dist < last or (dist == last and which == way)

    def w_copy(way, dist, number):
        part, cut = number // 2, pl.ds(number % 2 * quarter, quarter)
        to = slot(way, dist)
        return remote(
            wbuf.at[slot(way, dist - 1), part, :, cut],
            wbuf.at[to, part, :, cut],
            w_send.at[way, dist, number],
            w_recv.at[to, number],
            ring[way],
        )

    def w_goes(way, dist, number):
        return dist < last or (dist == last and number // 2 == way)

    def half_copy(number):
        cut = pl.ds(number * quarter, quarter)
        return remote(
            w_out.at[:, cut], wbuf.at[0, 1, :, cut], half_send.at[number], half_recv.at[number], {"head": partner}
        )

    def send_kv(dist):
        for way in range(2):
            for which in range(2):
                if kv_goes(which, way, dist):
                    start(kv_copy(which, way, dist))

    def wait_kv(dist):
        for way in range(2):
            for which in range(2):
                if kv_goes(which, way, dist):
                    kv_copy(which, way, dist).wait_recv()

    def send_w(dist, number):
        for way in range(2):
            if w_goes(way, dist, number):
                start(w_copy(way, dist, number))

    def pass_w(dist, number):
        for way in range(2):
            if w_goes(way, dist, number):
                w_copy(way, dist, number).wait_recv()
                if w_goes(way, dist + 1, number):
                    start(w_copy(way, dist + 1, number))

    fetches[0].wait()
    fetches[1].wait()
    send_kv(1)
    fetches[2].wait()
    for cut in range(2):
        start(half_copy(cut))
    fetches[3].wait()
    send_w(1, 0)
    for fetch in fetches[4:]:
        fetch.wait()

    down = lax.broadcasted_iota(jnp.int32, (span, span), 0)
    along = lax.broadcasted_iota(jnp.int32, (span, span), 1)
    query_at, query_doc = [], []
    for part in range(2):
        block = order_ref[2 * seq + part]
        query_at.append(down + block * span)
        docs = doc_ref[pl.ds(block, 1), :].astype(jnp.float32)
        query_doc.append(jnp.transpose(jnp.broadcast_to(docs, (span, span))))

    def mask(number):
        for j in range(2):
            block = order_ref[2 * origin(number) + j]
            docs = doc_ref[pl.ds(block, 1), :].astype(jnp.float32)
            key_at = along + block * span
            first = (2 * number + j) * span
            for part in range(2):
                seen = (query_doc[part] == docs) & (key_at <= query_at[part])
                bias[part, :, first : first + span] = jnp.where(seen, jnp.float32(0.0), jnp.float32(-1e30))

    mask(0)
    half_copy(0).wait_recv()
    send_w(1, 2)
    for dist in range(1, last + 1):
        wait_kv(dist)
        if dist < last:
            send_kv(dist + 1)
        if dist == 1:
            send_w(1, 1)
        if dist == 2:
            half_copy(1).wait_recv()
            send_w(1, 3)
        mask(slot(0, dist))
        if dist < last:
            mask(slot(1, dist))

    def attend(part, h):
        q = q_ref[part * span : (part + 1) * span, h * DH : (h + 1) * DH]
        keys = kbuf[...].reshape(n * rows, DH)
        scores = lax.dot_general(q, keys, (((1,), (1,)), ((), ())), preferred_element_type=jnp.float32)
        masked = scores * scale + bias[part]
        weights = jnp.exp(masked - jnp.max(masked, axis=-1, keepdims=True))
        total = jnp.sum(weights, axis=-1, keepdims=True)
        summed = jnp.dot(
            weights.astype(jnp.bfloat16), vbuf[...].reshape(n * rows, DH), preferred_element_type=jnp.float32
        )
        att[0, part * span : (part + 1) * span, h * DH : (h + 1) * DH] = (summed / total).astype(jnp.bfloat16)

    units = [(part, h) for part in range(2) for h in range(heads)]
    events = [(dist, number) for dist in range(1, last + 1) for number in pieces]
    cols_of = out_ref.shape[1] // width

    def target(number):
        block = origin(number)
        to = block // cols_of
        return block, to, 2 * ((pair + to // 2) % 2) + (core + to) % 2

    def sum_copy(number, cut):
        block, to, code = target(number)
        return remote(
            stage.at[number, cut],
            sums.at[code, block % cols_of, cut],
            sum_send.at[number, cut],
            sum_recv.at[code, block % cols_of, cut],
            {"head": to},
        )

    def project(number, cut):
        block, to, code = target(number)
        cols = slice(cut * quarter, (cut + 1) * quarter)
        added = jnp.dot(att[0], wbuf[number, 0, :, cols], preferred_element_type=jnp.float32)
        added = added + jnp.dot(att[1], wbuf[number, 1, :, cols], preferred_element_type=jnp.float32)

        @pl.when(code == 0)
        def _():
            kept[block % cols_of, cut] = added

        @pl.when(code != 0)
        def _():
            stage[number, cut] = added.astype(jnp.bfloat16)
            sum_copy(number, cut).start()

    def att_copy():
        return remote(att.at[0], att.at[1], att_send, att_recv, {"head": partner})

    ready = [(0, 0), (0, 1)]
    done_att = False
    for at, (dist, number) in enumerate(events):
        pass_w(dist, number)
        if number >= 2:
            cut = number % 2
            ready += [(slot(0, dist), cut)] + ([(slot(1, dist), cut)] if dist < last else [])
        if at >= len(pieces) - 1:
            for part, h in units[:2]:
                attend(part, h)
            units = units[2:]
        if not units and not done_att:
            start(att_copy())
            att_copy().wait_recv()
            done_att = True
        elif done_att:
            for _ in range(4):
                if ready:
                    project(*ready.pop(0))
    for item in ready:
        project(*item)

    own = pl.multiple_of(core * half, half)
    far = pl.multiple_of((1 - core) * half, half)
    for cut in range(2):
        for j in range(cols_of):
            for code in range(1, 4):
                remote(
                    stage.at[0, cut], sums.at[code, j, cut], sum_send.at[0, cut], sum_recv.at[code, j, cut], {"head": partner}
                ).wait_recv()
            at = j * width + cut * quarter
            out_ref[:, pl.ds(pl.multiple_of(at + own, quarter), quarter)] = (
                kept[j, cut] + sums[2, j, cut].astype(jnp.float32)
            ).astype(jnp.bfloat16)
            out_ref[:, pl.ds(pl.multiple_of(at + far, quarter), quarter)] = (
                sums[1, j, cut].astype(jnp.float32) + sums[3, j, cut].astype(jnp.float32)
            ).astype(jnp.bfloat16)
    for copy in sent:
        copy.wait_send()
    for number in range(n):

        @pl.when(target(number)[2] != 0)
        def _(number=number):
            for cut in range(2):
                sum_copy(number, cut).wait_send()


def ring_form(n, queries, keys, values, doc_ids, span_order, out_weight):
    rows = queries.shape[0]
    depth, width = out_weight.shape
    half = width // 2
    per_head = n // 4
    bf16 = jnp.bfloat16
    dma = pltpu.SemaphoreType.DMA
    return pl.pallas_call(
        functools.partial(ring_kernel, n),
        out_shape=jax.ShapeDtypeStruct((rows, width * per_head), bf16),
        in_specs=[pl.BlockSpec(memory_space=pl.ANY)] * 6,
        out_specs=pl.BlockSpec(memory_space=pltpu.VMEM),
        scratch_shapes=[
            pltpu.VMEM(queries.shape, bf16),
            pltpu.VMEM((doc_ids.shape[0] // (rows // 2), rows // 2), jnp.int32),
            pltpu.SMEM(span_order.shape, jnp.int32),
            pltpu.VMEM((depth, half), bf16),
            dma((7,)),
            pltpu.VMEM((n, rows, DH), bf16),
            pltpu.VMEM((n, rows, DH), bf16),
            pltpu.VMEM((n, 2, depth, half), bf16),
            pltpu.VMEM((2, rows // 2, n * rows), jnp.float32),
            pltpu.VMEM((2,) + queries.shape, bf16),
            pltpu.VMEM((n, 2, rows, half // 2), bf16),
            pltpu.VMEM((per_head, 2, rows, half // 2), jnp.float32),
            pltpu.VMEM((4, per_head, 2, rows, half // 2), bf16),
            dma((2, n // 2 + 1)),
            dma((n,)),
            dma((2, n // 2 + 1)),
            dma((n,)),
            dma((2, n // 2 + 1, 4)),
            dma((n, 4)),
            dma((2,)),
            dma((2,)),
            dma,
            dma,
            dma((n, 2)),
            dma((4, per_head, 2)),
        ],
        compiler_params=pltpu.CompilerParams(
            collective_id=0, has_side_effects=True, vmem_limit_bytes=62 * 1024 * 1024
        ),
    )(queries, keys, values, doc_ids.reshape(-1, rows // 2), span_order, out_weight)


def on_device(mesh_shape, queries, keys, values, doc_ids, span_order, out_weight):
    n, groups = mesh_shape["seq"], mesh_shape["head"]
    rows = queries.shape[0]
    depth, width = out_weight.shape
    held = n * (depth * width + 2 * rows * DH) * 2
    fits = (
        groups == 4
        and n % 4 == 0
        and rows == 2 * DH
        and keys.shape[1] == DH
        and width % (4 * DH) == 0
        and held <= 16 * 1024 * 1024
    )
    if fits:
        return ring_form(n, queries, keys, values, doc_ids, span_order, out_weight)
    return gathered_form(queries, keys, values, doc_ids, span_order, out_weight)


def solution(mesh):
    return jax.shard_map(
        functools.partial(on_device, dict(mesh.shape)),
        mesh=mesh,
        in_specs=(P("seq", "head"), P("seq", "head"), P("seq", "head"), P(), P(), P("head", "seq")),
        out_specs=P("seq", "head"),
        check_vma=False,
    )
```

```python
import functools
import math

import jax
import jax.numpy as jnp
from jax import lax
from jax.experimental import pallas as pl
from jax.experimental.pallas import tpu as pltpu
from jax.sharding import PartitionSpec as P

MESH = pl.DeviceIdType.MESH

DH = 128


def gathered_form(queries, keys, values, doc_ids, span_order, out_weight):
    tok_rows = queries.shape[0]
    span = tok_rows // 2
    local_heads = queries.shape[1] // DH
    local_kv = keys.shape[1] // DH
    group_size = local_heads // local_kv
    n_blocks = span_order.shape[0]
    scale = 1.0 / math.sqrt(DH)
    mine = lax.axis_index("seq")
    own_blocks = lax.dynamic_slice_in_dim(span_order, 2 * mine, 2, 0)
    local_rows = jnp.arange(tok_rows, dtype=jnp.int32)
    qpos = jnp.where(local_rows < span, own_blocks[0], own_blocks[1]) * span + local_rows % span
    qdoc = jnp.take(doc_ids, qpos)
    q_heads = queries.reshape(tok_rows, local_kv, group_size, DH)

    def update(state, kblk, vblk, kpos, kdoc):
        largest, total, summed = state
        count = kblk.shape[0]
        k_heads = kblk.reshape(count, local_kv, DH)
        v_heads = vblk.reshape(count, local_kv, DH)
        scores = (
            jnp.einsum("qhgd,khd->hgqk", q_heads, k_heads, preferred_element_type=jnp.float32)
            * scale
        )
        visible = (qdoc[:, None] == kdoc[None, :]) & (kpos[None, :] <= qpos[:, None])
        masked = jnp.where(visible, scores, jnp.float32(-1e30))
        new_largest = jnp.maximum(largest, jnp.max(masked, axis=-1))
        factor = jnp.exp(largest - new_largest)
        weights = jnp.where(visible, jnp.exp(masked - new_largest[..., None]), jnp.float32(0.0))
        total = total * factor + jnp.sum(weights, axis=-1)
        weights_b = weights.astype(jnp.bfloat16)
        added = jnp.einsum("hgqk,khd->qhgd", weights_b, v_heads, preferred_element_type=jnp.float32)
        summed = summed * jnp.transpose(factor, (2, 0, 1))[..., None] + added
        return (new_largest, total, summed)

    initial = (
        jnp.full((local_kv, group_size, tok_rows), -1e30, jnp.float32),
        jnp.zeros((local_kv, group_size, tok_rows), jnp.float32),
        jnp.zeros((tok_rows, local_kv, group_size, DH), jnp.float32),
    )
    state = initial
    kpiece = lax.all_gather(keys, "seq", axis=0, tiled=True)
    vpiece = lax.all_gather(values, "seq", axis=0, tiled=True)
    count = kpiece.shape[0]
    width = math.gcd(count, 1024)
    steps = count // width
    rows = jnp.arange(count, dtype=jnp.int32)
    match = (rows // span)[:, None] == jnp.arange(n_blocks, dtype=jnp.int32)[None, :]
    owner = jnp.sum(jnp.where(match, span_order[None, :], 0), axis=1)
    kpos = owner * span + rows % span
    kdoc = jnp.take(doc_ids, kpos)
    kparts = kpiece.reshape(steps, width, kpiece.shape[1])
    vparts = vpiece.reshape(steps, width, vpiece.shape[1])

    def one_step(carry, items):
        kblk, vblk, pblk, dblk = items
        carry = update(carry, kblk, vblk, pblk, dblk)
        return (carry, None)

    state, unused = lax.scan(
        one_step, state, (kparts, vparts, kpos.reshape(steps, width), kdoc.reshape(steps, width))
    )
    largest, total, summed = state
    attended = (summed / jnp.transpose(total, (2, 0, 1))[..., None]).astype(jnp.bfloat16)
    attended = attended.reshape(tok_rows, local_heads * DH)
    partial_out = jnp.dot(
        attended,
        lax.all_gather(out_weight, "seq", axis=1, tiled=True),
        preferred_element_type=jnp.float32,
    )
    return lax.psum_scatter(
        partial_out.astype(jnp.bfloat16), "head", scatter_dimension=1, tiled=True
    )


def ring_kernel(
    n, q_in, k_in, v_in, doc_in, order_in, w_in, out_ref,
    q_ref, doc_ref, order_ref, w_out, fetched, kbuf, vbuf, wbuf, bias, att, stage, kept, sums,
    k_send, k_recv, v_send, v_recv, w_send, w_recv, half_send, half_recv,
    att_send, att_recv, sum_send, sum_recv,
):
    seq = lax.axis_index("seq")
    head = lax.axis_index("head")
    pair, core = head // 2, head % 2
    partner = 2 * pair + 1 - core
    last = n // 2
    rows = q_ref.shape[0]
    span = rows // 2
    heads = q_ref.shape[1] // DH
    width = w_in.shape[1]
    half = width // 2
    quarter = half // 2
    pieces = (0, 2, 1, 3)
    scale = 1.0 / math.sqrt(DH)

    def seq_at(place):
        low = place // last
        return (1 - low) * 2 * place + low * (2 * (n - 1 - place) + 1)

    odd = seq % 2
    place = (1 - odd) * (seq // 2) + odd * (n - 1 - seq // 2)
    right, left = seq_at((place + 1) % n), seq_at((place + n - 1) % n)
    ring = ({"seq": right}, {"seq": left})

    def slot(way, dist):
        if dist == 0:
            return 0
        if dist == last:
            return n - 1
        return dist if way == 0 else last - 1 + dist

    def origin(number):
        if number < last:
            return seq_at((place + n - number) % n)
        if number == n - 1:
            return seq_at((place + last) % n)
        return seq_at((place + number - last + 1) % n)

    mine = pl.ds(pl.multiple_of(core * half, half), half)
    theirs = pl.ds(pl.multiple_of((1 - core) * half, half), half)
    fetches = [
        pltpu.make_async_copy(src, dst, fetched.at[at])
        for at, (src, dst) in enumerate(
            (
                (k_in, kbuf.at[0]),
                (v_in, vbuf.at[0]),
                (w_in.at[:, theirs], w_out),
                (w_in.at[:, mine], wbuf.at[0, 0]),
                (doc_in, doc_ref),
                (order_in, order_ref),
                (q_in, q_ref),
            )
        )
    ]
    for fetch in fetches:
        fetch.start()

    barrier = pltpu.get_barrier_semaphore()
    other = (pair + 1) % 2
    greet = ring + ({"head": partner}, {"head": 2 * other}, {"head": 2 * other + 1})
    for device in greet:
        pl.semaphore_signal(barrier, inc=1, device_id=device, device_id_type=MESH)
    pl.semaphore_wait(barrier, len(greet))

    sent = []

    def start(copy):
        copy.start()
        sent.append(copy)

    def remote(src, dst, send, recv, device):
        return pltpu.make_async_remote_copy(
            src_ref=src, dst_ref=dst, send_sem=send, recv_sem=recv, device_id=device, device_id_type=MESH
        )

    def kv_copy(which, way, dist):
        buf, ss, rs = ((kbuf, k_send, k_recv), (vbuf, v_send, v_recv))[which]
        to = slot(way, dist)
        return remote(buf.at[slot(way, dist - 1)], buf.at[to], ss.at[way, dist], rs.at[to], ring[way])

    def kv_goes(which, way, dist):
        return dist < last or (dist == last and which == way)

    def w_copy(way, dist, number):
        part, cut = number // 2, pl.ds(number % 2 * quarter, quarter)
        to = slot(way, dist)
        return remote(
            wbuf.at[slot(way, dist - 1), part, :, cut],
            wbuf.at[to, part, :, cut],
            w_send.at[way, dist, number],
            w_recv.at[to, number],
            ring[way],
        )

    def w_goes(way, dist, number):
        return dist < last or (dist == last and number // 2 == way)

    def half_copy(number):
        cut = pl.ds(number * quarter, quarter)
        return remote(
            w_out.at[:, cut], wbuf.at[0, 1, :, cut], half_send.at[number], half_recv.at[number], {"head": partner}
        )

    def send_kv(dist):
        for way in range(2):
            for which in range(2):
                if kv_goes(which, way, dist):
                    start(kv_copy(which, way, dist))

    def pass_kv(dist):
        for which in range(2):
            for way in range(2):
                if kv_goes(which, way, dist):
                    kv_copy(which, way, dist).wait_recv()
                    if kv_goes(which, way, dist + 1):
                        start(kv_copy(which, way, dist + 1))

    def send_w(dist, number):
        for way in range(2):
            if w_goes(way, dist, number):
                start(w_copy(way, dist, number))

    def pass_w(dist, number):
        for way in range(2):
            if w_goes(way, dist, number):
                w_copy(way, dist, number).wait_recv()
                if w_goes(way, dist + 1, number):
                    start(w_copy(way, dist + 1, number))

    fetches[0].wait()
    fetches[1].wait()
    send_kv(1)
    fetches[2].wait()
    for cut in range(2):
        start(half_copy(cut))
    fetches[3].wait()
    send_w(1, 0)
    for fetch in fetches[4:]:
        fetch.wait()

    down = lax.broadcasted_iota(jnp.int32, (span, span), 0)
    along = lax.broadcasted_iota(jnp.int32, (span, span), 1)
    query_at, query_doc = [], []
    for part in range(2):
        block = order_ref[2 * seq + part]
        query_at.append(down + block * span)
        docs = doc_ref[pl.ds(block, 1), :].astype(jnp.float32)
        query_doc.append(jnp.transpose(jnp.broadcast_to(docs, (span, span))))

    def mask(number):
        for j in range(2):
            block = order_ref[2 * origin(number) + j]
            docs = doc_ref[pl.ds(block, 1), :].astype(jnp.float32)
            key_at = along + block * span
            first = (2 * number + j) * span
            for part in range(2):
                seen = (query_doc[part] == docs) & (key_at <= query_at[part])
                bias[part, :, first : first + span] = jnp.where(seen, jnp.float32(0.0), jnp.float32(-1e30))

    mask(0)
    half_copy(0).wait_recv()
    send_w(1, 2)
    for dist in range(1, last + 1):
        pass_kv(dist)
        if dist == 1:
            send_w(1, 1)
        if dist == 2:
            half_copy(1).wait_recv()
            send_w(1, 3)
        if dist == last - 1:
            pass_w(1, pieces[0])
        mask(slot(0, dist))
        if dist < last:
            mask(slot(1, dist))

    def attend(part, h):
        q = q_ref[part * span : (part + 1) * span, h * DH : (h + 1) * DH]
        keys = kbuf[...].reshape(n * rows, DH)
        scores = lax.dot_general(q, keys, (((1,), (1,)), ((), ())), preferred_element_type=jnp.float32)
        masked = scores * scale + bias[part]
        weights = jnp.exp(masked - jnp.max(masked, axis=-1, keepdims=True))
        total = jnp.sum(weights, axis=-1, keepdims=True)
        summed = jnp.dot(
            weights.astype(jnp.bfloat16), vbuf[...].reshape(n * rows, DH), preferred_element_type=jnp.float32
        )
        att[0, part * span : (part + 1) * span, h * DH : (h + 1) * DH] = (summed / total).astype(jnp.bfloat16)

    units = [(part, h) for part in range(2) for h in range(heads)]
    events = [(dist, number) for dist in range(1, last + 1) for number in pieces]
    cols_of = out_ref.shape[1] // width

    def target(number):
        block = origin(number)
        to = block // cols_of
        return block, to, 2 * ((pair + to // 2) % 2) + (core + to) % 2

    def sum_copy(number, cut):
        block, to, code = target(number)
        return remote(
            stage.at[number, cut],
            sums.at[code, block % cols_of, cut],
            sum_send.at[number, cut],
            sum_recv.at[code, block % cols_of, cut],
            {"head": to},
        )

    def project(number, cut):
        block, to, code = target(number)
        cols = slice(cut * quarter, (cut + 1) * quarter)
        added = jnp.dot(att[0], wbuf[number, 0, :, cols], preferred_element_type=jnp.float32)
        added = added + jnp.dot(att[1], wbuf[number, 1, :, cols], preferred_element_type=jnp.float32)

        @pl.when(code == 0)
        def _():
            kept[block % cols_of, cut] = added

        @pl.when(code != 0)
        def _():
            stage[number, cut] = added.astype(jnp.bfloat16)
            sum_copy(number, cut).start()

    def att_copy():
        return remote(att.at[0], att.at[1], att_send, att_recv, {"head": partner})

    ready = [(0, 0), (0, 1)]
    att_step = 0
    for at, (dist, number) in enumerate(events):
        if at > 0:
            pass_w(dist, number)
        if number >= 2:
            cut = number % 2
            ready += [(slot(0, dist), cut)] + ([(slot(1, dist), cut)] if dist < last else [])
        if at >= len(pieces) - 1:
            for part, h in units[:2]:
                attend(part, h)
            units = units[2:]
        if not units:
            att_step += 1
            if att_step == 1:
                start(att_copy())
            if att_step == 2:
                att_copy().wait_recv()
        if att_step > 1:
            for _ in range(4):
                if ready:
                    project(*ready.pop(0))
    for item in ready:
        project(*item)

    own = pl.multiple_of(core * half, half)
    far = pl.multiple_of((1 - core) * half, half)
    for cut in range(2):
        for j in range(cols_of):
            for code in range(1, 4):
                remote(
                    stage.at[0, cut], sums.at[code, j, cut], sum_send.at[0, cut], sum_recv.at[code, j, cut], {"head": partner}
                ).wait_recv()
            at = j * width + cut * quarter
            out_ref[:, pl.ds(pl.multiple_of(at + own, quarter), quarter)] = (
                kept[j, cut] + sums[2, j, cut].astype(jnp.float32)
            ).astype(jnp.bfloat16)
            out_ref[:, pl.ds(pl.multiple_of(at + far, quarter), quarter)] = (
                sums[1, j, cut].astype(jnp.float32) + sums[3, j, cut].astype(jnp.float32)
            ).astype(jnp.bfloat16)
    for copy in sent:
        copy.wait_send()
    for number in range(n):

        @pl.when(target(number)[2] != 0)
        def _(number=number):
            for cut in range(2):
                sum_copy(number, cut).wait_send()


def ring_form(n, queries, keys, values, doc_ids, span_order, out_weight):
    rows = queries.shape[0]
    depth, width = out_weight.shape
    half = width // 2
    per_head = n // 4
    bf16 = jnp.bfloat16
    dma = pltpu.SemaphoreType.DMA
    return pl.pallas_call(
        functools.partial(ring_kernel, n),
        out_shape=jax.ShapeDtypeStruct((rows, width * per_head), bf16),
        in_specs=[pl.BlockSpec(memory_space=pl.ANY)] * 6,
        out_specs=pl.BlockSpec(memory_space=pltpu.VMEM),
        scratch_shapes=[
            pltpu.VMEM(queries.shape, bf16),
            pltpu.VMEM((doc_ids.shape[0] // (rows // 2), rows // 2), jnp.int32),
            pltpu.SMEM(span_order.shape, jnp.int32),
            pltpu.VMEM((depth, half), bf16),
            dma((7,)),
            pltpu.VMEM((n, rows, DH), bf16),
            pltpu.VMEM((n, rows, DH), bf16),
            pltpu.VMEM((n, 2, depth, half), bf16),
            pltpu.VMEM((2, rows // 2, n * rows), jnp.float32),
            pltpu.VMEM((2,) + queries.shape, bf16),
            pltpu.VMEM((n, 2, rows, half // 2), bf16),
            pltpu.VMEM((per_head, 2, rows, half // 2), jnp.float32),
            pltpu.VMEM((4, per_head, 2, rows, half // 2), bf16),
            dma((2, n // 2 + 1)),
            dma((n,)),
            dma((2, n // 2 + 1)),
            dma((n,)),
            dma((2, n // 2 + 1, 4)),
            dma((n, 4)),
            dma((2,)),
            dma((2,)),
            dma,
            dma,
            dma((n, 2)),
            dma((4, per_head, 2)),
        ],
        compiler_params=pltpu.CompilerParams(
            collective_id=0, has_side_effects=True, vmem_limit_bytes=62 * 1024 * 1024
        ),
    )(queries, keys, values, doc_ids.reshape(-1, rows // 2), span_order, out_weight)


def on_device(mesh_shape, queries, keys, values, doc_ids, span_order, out_weight):
    n, groups = mesh_shape["seq"], mesh_shape["head"]
    rows = queries.shape[0]
    depth, width = out_weight.shape
    held = n * (depth * width + 2 * rows * DH) * 2
    fits = (
        groups == 4
        and n % 4 == 0
        and rows == 2 * DH
        and keys.shape[1] == DH
        and width % (4 * DH) == 0
        and held <= 16 * 1024 * 1024
    )
    if fits:
        return ring_form(n, queries, keys, values, doc_ids, span_order, out_weight)
    return gathered_form(queries, keys, values, doc_ids, span_order, out_weight)


def solution(mesh):
    return jax.shard_map(
        functools.partial(on_device, dict(mesh.shape)),
        mesh=mesh,
        in_specs=(P("seq", "head"), P("seq", "head"), P("seq", "head"), P(), P(), P("head", "seq")),
        out_specs=P("seq", "head"),
        check_vma=False,
    )
```
